32 devices in a mesh: row: 8 (over z, core), col: 4 (over y, x).
Axes of the slice: x: 2, y: 2, z: 4, core: 2. Of those that a mesh axis runs over, the one named last changes fastest.
Arguments:
- attn_out: bfloat16 [6, 512, 2048], P(None, 'col', 'row'), may hold values from -0.625 to 0.625
- out_cotangent: bfloat16 [6, 512, 2048], P(None, 'row', 'col'), may hold values from -6 to 6
- frozen: bfloat16 [6, 2048, 2048], P(None, 'row', 'col'), may hold values from -0.5 to 0.5
- adapt_in: bfloat16 [6, 32, 2048], P(None, None, 'row'), may hold values from -0.125 to 0.125
- adapt_out: bfloat16 [6, 32, 2048], P(None, None, 'col'), may hold values from -1 to 1
- magnitude: float32 [6, 2048], P(None, 'col'), may hold values from 0.1 to 1.9
Outputs:
- input_grad: bfloat16 [6, 512, 2048], P(None, 'col', 'row')
- adapt_in_grad: float32 [6, 32, 2048], P(None, None, 'row')
- adapt_out_grad: float32 [6, 32, 2048], P(None, None, 'col')
- magnitude_grad: float32 [6, 2048], P(None, 'col')
The draws below stay inside these ranges and needn't reach their ends.
All inputs are finite; a program needn't handle non-finite values.
Results may differ from the reference program's by a relative error of at most 0.0065.
Values may be sent and summed in bfloat16 or wider, within the bound.
No kernel may reach another device: no remote copies, remote signals or barrier semaphores. Data moves between devices by JAX's collectives and lax.ppermute only.
A program may use at most 64 MiB of HBM per device.

```python
import jax
import jax.numpy as jnp
from jax import lax

WIDTH = 2048
IN_WIDTH = 2048
RANK = 32
LAYERS = 6
TOKENS = 512


def steps_of(key, extent, shards, smallest, top_value):
    def one(dim, shards_of):
        steps = jax.random.uniform(jax.random.fold_in(jax.random.fold_in(key, 6), dim), (shards_of,), jnp.float32, smallest / len(shards), top_value / len(shards))
        return jnp.repeat(jnp.exp(steps), extent[dim] // shards_of).reshape((-1,) + (1,) * (len(extent) - dim - 1))

    level = one(*shards[0])
    for cut in shards[1:]:
        level = level * one(*cut)
    return level


def gaussian(rng, extent, spread, reach, split=(), kind=jnp.bfloat16):
    level = steps_of(rng, extent, split, -0.22, 0.18) if split else 1.0
    entries = jax.random.normal(rng, extent, jnp.float32) * spread * level
    return jnp.minimum(jnp.maximum(entries, -reach), reach).astype(kind)


def setup_inputs(seed: int = 0) -> dict:
    key_list = jax.random.split(jax.random.key(seed), 7)
    attn_out = gaussian(key_list[0], (LAYERS, TOKENS, IN_WIDTH), (TOKENS ** -0.5), 0.625, ((1, 4), (2, 8)))
    out_cotangent = gaussian(key_list[1], (LAYERS, TOKENS, WIDTH), 1.0, 6.0, ((1, 8), (2, 4)))
    frozen = gaussian(key_list[2], (LAYERS, IN_WIDTH, WIDTH), (IN_WIDTH // 16) ** -0.5, 0.5, ((1, 8), (2, 4)))
    adapt_in = gaussian(key_list[3], (LAYERS, RANK, IN_WIDTH), IN_WIDTH ** -0.5, 0.125, ((2, 8),))
    adapt_out = gaussian(key_list[4], (LAYERS, RANK, WIDTH), RANK ** -0.5, 1.0, ((2, 4),))
    magnitude = jnp.clip(1.0 + 0.18 * jax.random.normal(key_list[5], (LAYERS, WIDTH), jnp.float32), 0.1, 1.9)
    return {"attn_out": attn_out, "out_cotangent": out_cotangent, "frozen": frozen, "adapt_in": adapt_in, "adapt_out": adapt_out, "magnitude": magnitude}


precise = lax.Precision.HIGHEST

def one_layer(acts, grads, frozen, adapt_in, adapt_out, magnitude):
    merged = frozen.astype(jnp.float32) + lax.dot_general(adapt_in, adapt_out, (((0,), (0,)), ((), ())), preferred_element_type=jnp.float32)
    squares = lax.optimization_barrier(jnp.sum(merged * merged, axis=0))
    norms = jnp.sqrt(squares + 0.25)
    outer = lax.dot_general(acts, grads, (((0,), (0,)), ((), ())), preferred_element_type=jnp.float32)
    dots = lax.optimization_barrier(jnp.sum(merged * outer, axis=0))
    scales = magnitude / norms
    correct = -magnitude * dots / (norms * norms * norms)
    magnitude_grad = dots / norms
    delta = outer * scales + merged * correct
    in_grad = lax.dot_general(adapt_out.astype(jnp.float32), delta, (((1,), (1,)), ((), ())), precision=precise)
    out_grad = jnp.dot(adapt_in.astype(jnp.float32), delta, precision=precise)
    scaled = (grads * scales).astype(jnp.bfloat16)
    weight_low = merged.astype(jnp.bfloat16)
    input_grad = lax.dot_general(scaled, weight_low, (((1,), (1,)), ((), ())), preferred_element_type=jnp.float32).astype(jnp.bfloat16)
    return (input_grad, in_grad, out_grad, magnitude_grad)

def reference(attn_out, out_cotangent, frozen, adapt_in, adapt_out, magnitude):
    results = [one_layer(attn_out[layer_at], out_cotangent[layer_at], frozen[layer_at], adapt_in[layer_at], adapt_out[layer_at], magnitude[layer_at]) for layer_at in range(LAYERS)]
    return (jnp.stack([item[0] for item in results]), jnp.stack([item[1] for item in results]), jnp.stack([item[2] for item in results]), jnp.stack([item[3] for item in results]))
```

```python
import jax
import jax.numpy as jnp
from jax import lax
from jax.experimental import pallas as pl
from jax.experimental.pallas import tpu as pltpu
from jax.sharding import PartitionSpec as P


f32 = jnp.float32
bf16 = jnp.bfloat16


def dot(a, b, ca, cb):
    return lax.dot_general(a, b, (((ca,), (cb,)), ((), ())), preferred_element_type=f32)


def merged_of(frozen, adapt_in, adapt_out):
    return frozen[...].astype(f32) + dot(adapt_in[...], adapt_out[...], 0, 0)


def split_dot(a, b, ca, cb):
    high = b.astype(bf16)
    low = (b - high.astype(f32)).astype(bf16)
    return dot(a, high, ca, cb) + dot(a, low, ca, cb)


def weight_stats(frozen, adapt_in, adapt_out, squares, inner):
    merged = merged_of(frozen, adapt_in, adapt_out)
    squares[...] = jnp.sum(merged * merged, axis=0, keepdims=True)
    inner[...] = split_dot(adapt_in[...], merged, 1, 0)


def fill(spots, pieces, whole):
    rows = pieces[0].shape[0]
    for at, piece in enumerate(pieces):
        whole[pl.ds(pl.multiple_of(spots[at] * rows, rows), rows), :] = piece[...]


def input_part(count, blocks, spots, *refs):
    pieces = refs[:count]
    frozen, adapt_in, adapt_out, scales = refs[count : count + 4]
    outs = refs[count + 4 : count + 4 + blocks]
    grads = refs[-1]
    fill(spots, pieces, grads)
    weight = (merged_of(frozen, adapt_in, adapt_out) * scales[...]).astype(bf16)
    for at, out in enumerate(outs):
        rows = out.shape[0]
        block = grads[pl.ds(pl.multiple_of(spots[count + at] * rows, rows), rows), :]
        out[...] = dot(block, weight, 1, 1).astype(bf16)


def outer_part(count, blocks, spots, *refs):
    pieces = refs[:count]
    act_pieces = refs[count : count + blocks]
    frozen, adapt_in, adapt_out, scales = refs[count + blocks : count + blocks + 4]
    dots, inner, in_part, grads, acts = refs[count + blocks + 4 :]
    fill(spots, pieces, grads)
    rows = act_pieces[0].shape[0]
    for at, piece in enumerate(act_pieces):
        acts[pl.ds(pl.multiple_of(spots[count + at] * rows, rows), rows), :] = piece[...]
    outer = dot(acts[...], grads[...], 0, 0)
    merged = merged_of(frozen, adapt_in, adapt_out)
    dots[...] = jnp.sum(merged * outer, axis=0, keepdims=True)
    inner[...] = split_dot(adapt_in[...], outer, 1, 0)
    in_part[...] = split_dot(adapt_out[...], outer * scales[...], 1, 1)


def correct_part(frozen, adapt_in, adapt_out, correct, in_part, out):
    merged = merged_of(frozen, adapt_in, adapt_out)
    out[...] = (in_part[...] + split_dot(adapt_out[...], merged * correct[...], 1, 1)).astype(out.dtype)


def layer_block(array, start=0):
    return pl.BlockSpec((None,) + array.shape[1:], lambda at, *_: (at + start, 0, 0))


def call(kernel, layers, spots, inputs, outs, scratch=()):
    grid_spec = pltpu.PrefetchScalarGridSpec(
        num_scalar_prefetch=0 if spots is None else 1,
        grid=(layers,),
        in_specs=[layer_block(array, start) for array, start in inputs],
        out_specs=[layer_block(out) for out in outs],
        scratch_shapes=list(scratch),
    )
    first = () if spots is None else (spots,)
    return pl.pallas_call(kernel, grid_spec=grid_spec, out_shape=list(outs))(
        *first, *[array for array, _ in inputs]
    )


def make_body(rows, cols):
    zs = rows // 2
    mate = [(r, r ^ 1) for r in range(rows)]

    def along(shift):
        return [(r, (r + 2 * shift) % rows) for r in range(rows)]

    def send(x, perm):
        return lax.ppermute(x, "row", perm)

    def cross(x, k):
        return lax.ppermute(x, "col", [(c, c ^ k) for c in range(cols)])

    def tree(parts):
        while len(parts) > 1:
            parts = [sum(parts[at : at + 2][1:], parts[at]) for at in range(0, len(parts), 2)]
        return parts[0]

    def over_z(x):
        perms = [[(r, r ^ (2 * k)) for r in range(rows)] for k in range(1, zs)]
        return tree([x.astype(f32)] + [send(x, perm).astype(f32) for perm in perms])

    def over_col(x):
        return tree([x.astype(f32)] + [cross(x, k).astype(f32) for k in range(1, cols)])

    def row_sum(x):
        return over_z(x + send(x, mate))

    def body(attn_out, out_cotangent, frozen, adapt_in, adapt_out, magnitude):
        layers, in_block, out_block = frozen.shape
        rank = adapt_in.shape[1]
        tokens = attn_out.shape[1] * cols
        mid = layers // 2
        row = lax.axis_index("row")
        col = lax.axis_index("col")
        core = row % 2
        z = row // 2
        halves = (slice(0, mid), slice(mid, layers))

        ups = [[out_cotangent[h]] for h in halves]
        downs = [[out_cotangent[h]] for h in halves]
        for step in range(1, zs // 2 + 1):
            last = step == zs // 2
            for h in (0, 1):
                if not last or h == 0:
                    ups[h].append(send(ups[h][-1], along(1)))
                if not last or h == 1:
                    downs[h].append(send(downs[h][-1], along(-1)))
        acts = [[attn_out[h] for h in halves]]
        for k in range(1, cols):
            got = cross(attn_out, k)
            acts.append([got[h] for h in halves])

        weights = (frozen, adapt_in, adapt_out)
        squares, inner_merged = call(
            weight_stats,
            layers,
            None,
            [(w, 0) for w in weights],
            [
                jax.ShapeDtypeStruct((layers, 1, out_block), f32),
                jax.ShapeDtypeStruct((layers, rank, out_block), f32),
            ],
        )
        squares = row_sum(squares)
        norms = jnp.sqrt(squares + 0.25)
        scales = magnitude[:, None, :] / norms

        halves_pieces = []
        spots = None
        for h in (0, 1):
            pieces, places = [], []
            for at, piece in enumerate(ups[h]):
                pieces.append(piece)
                places.append((z - at) % zs)
            for at, piece in enumerate(downs[h][1:]):
                pieces.append(piece)
                places.append((z + at + 1) % zs)
            both = pieces + [send(piece, mate) for piece in pieces]
            spots = [p * 2 + core for p in places] + [p * 2 + 1 - core for p in places]
            spots = spots + [col ^ k for k in range(cols)]
            halves_pieces.append((both, jnp.stack(spots).astype(jnp.int32)))

        grads_scratch = pltpu.VMEM((tokens, out_block), bf16)
        acts_scratch = pltpu.VMEM((tokens, in_block), bf16)
        token_block = tokens // cols
        input_halves, rest = [], []
        for h in (0, 1):
            pieces, spots = halves_pieces[h]
            start = halves[h].start
            count = halves[h].stop - start
            shared = [(w, start) for w in weights] + [(scales, start)]

            def one(kernel, inputs, outs, scratch):
                return call(
                    lambda *refs: kernel(len(pieces), cols, *refs), count, spots, inputs, outs, scratch
                )

            parts = one(
                input_part,
                [(p, 0) for p in pieces] + shared,
                [jax.ShapeDtypeStruct((count, token_block, in_block), bf16)] * cols,
                [grads_scratch],
            )
            total = parts[0].astype(f32)
            for k in range(1, cols):
                total = total + cross(parts[k], k).astype(f32)
            input_halves.append(total.astype(bf16))
            rest.append(
                one(
                    outer_part,
                    [(p, 0) for p in pieces] + [(a[h], 0) for a in acts] + shared,
                    [
                        jax.ShapeDtypeStruct((count, 1, out_block), f32),
                        jax.ShapeDtypeStruct((count, rank, out_block), f32),
                        jax.ShapeDtypeStruct((count, rank, in_block), f32),
                    ],
                    [grads_scratch, acts_scratch],
                )
            )
        dots, inner_outer, in_part = [jnp.concatenate(pair, 0) for pair in zip(*rest)]
        dots = row_sum(dots)
        correct = -magnitude[:, None, :] * dots / (norms * norms * norms)
        magnitude_grad = (dots / norms)[:, 0]

        half = rank // 2
        inner = jnp.concatenate([inner_outer[:, None], inner_merged[:, None]], 1)
        low, high = inner[:, :, :half], inner[:, :, half:]
        kept = jnp.where(core == 0, low, high)
        given = jnp.where(core == 0, high, low)
        kept = kept + send(given, mate)
        kept = over_z(kept.astype(bf16))
        mine = kept[:, 0] * scales + kept[:, 1] * correct
        other = send(mine, mate)
        out_grad = jnp.where(
            core == 0, jnp.concatenate([mine, other], 1), jnp.concatenate([other, mine], 1)
        )

        (in_part,) = call(
            correct_part,
            layers,
            None,
            [(w, 0) for w in weights] + [(correct, 0), (in_part, 0)],
            [jax.ShapeDtypeStruct((layers, rank, in_block), bf16)],
        )
        in_grad = over_col(in_part)
        return jnp.concatenate(input_halves, 0), in_grad, out_grad, magnitude_grad

    return body


def solution(mesh):
    return jax.shard_map(
        make_body(mesh.shape["row"], mesh.shape["col"]),
        mesh=mesh,
        in_specs=(
            P(None, "col", "row"),
            P(None, "row", "col"),
            P(None, "row", "col"),
            P(None, None, "row"),
            P(None, None, "col"),
            P(None, "col"),
        ),
        out_specs=(
            P(None, "col", "row"),
            P(None, None, "row"),
            P(None, None, "col"),
            P(None, "col"),
        ),
        check_vma=False,
    )
```

```python
import jax
import jax.numpy as jnp
from jax import lax
from jax.experimental import pallas as pl
from jax.experimental.pallas import tpu as pltpu
from jax.sharding import PartitionSpec as P


f32 = jnp.float32
bf16 = jnp.bfloat16


def dot(a, b, ca, cb):
    return lax.dot_general(a, b, (((ca,), (cb,)), ((), ())), preferred_element_type=f32)


def merged_of(frozen, adapt_in, adapt_out):
    return frozen[...].astype(f32) + dot(adapt_in[...], adapt_out[...], 0, 0)


def weight_stats(frozen, adapt_in, adapt_out, squares):
    merged = merged_of(frozen, adapt_in, adapt_out)
    squares[...] = jnp.sum(merged * merged, axis=0, keepdims=True)


def fill(spots, first, pieces, whole):
    rows = pieces[0].shape[0]
    for at, piece in enumerate(pieces):
        whole[pl.ds(pl.multiple_of(spots[first + at] * rows, rows), rows), :] = piece[...]


def token_part(count, blocks, spots, *refs):
    pieces, refs = refs[:count], refs[count:]
    act_pieces, refs = refs[:blocks], refs[blocks:]
    frozen, adapt_in, adapt_out, scales = refs[:4]
    outs = refs[4 : 4 + blocks]
    dots, kept, given, in_part, grads, acts, product, inner = refs[4 + blocks :]
    fill(spots, 0, pieces, grads)
    fill(spots, count, act_pieces, acts)
    merged = merged_of(frozen, adapt_in, adapt_out)
    weight = (merged * scales[...]).astype(bf16)
    product[...] = dot(grads[...], weight, 1, 1)
    for at, out in enumerate(outs):
        rows = out.shape[0]
        block = pl.ds(pl.multiple_of(spots[count + at] * rows, rows), rows)
        out[...] = product[block, :].astype(bf16)
    outer = dot(acts[...], grads[...], 0, 0)
    dots[...] = jnp.sum(merged * outer, axis=0, keepdims=True)
    inner[0] = dot(adapt_in[...], outer.astype(bf16), 1, 0)
    inner[1] = dot(adapt_in[...], merged.astype(bf16), 1, 0)
    half = inner.shape[1] // 2
    core = spots[count + blocks]
    for at in range(2):
        kept[at] = inner[at, pl.ds(pl.multiple_of(core * half, half), half), :]
        away = inner[at, pl.ds(pl.multiple_of((1 - core) * half, half), half), :]
        given[at] = away.astype(bf16)
    in_part[...] = dot(adapt_out[...], (outer * scales[...]).astype(bf16), 1, 1)


def correct_part(frozen, adapt_in, adapt_out, correct, in_part, out):
    merged = merged_of(frozen, adapt_in, adapt_out)
    out[...] = (in_part[...] + dot(adapt_out[...], (merged * correct[...]).astype(bf16), 1, 1)).astype(out.dtype)


def layer_block(array, step):
    return pl.BlockSpec((step,) + array.shape[1:], lambda at, *_: (at,) + (0,) * (len(array.shape) - 1))


def call(kernel, layers, spots, inputs, outs, scratch=()):
    step = layers // 2 if layers % 2 == 0 else 1
    first = 0 if spots is None else 1
    many = len(inputs) + len(outs)

    def steps(*refs):
        for at in range(step):
            kernel(
                *refs[:first],
                *[ref.at[at] for ref in refs[first : first + many]],
                *refs[first + many :],
            )

    grid_spec = pltpu.PrefetchScalarGridSpec(
        num_scalar_prefetch=first,
        grid=(layers // step,),
        in_specs=[layer_block(array, step) for array in inputs],
        out_specs=[layer_block(out, step) for out in outs],
        scratch_shapes=list(scratch),
    )
    return pl.pallas_call(steps, grid_spec=grid_spec, out_shape=list(outs))(
        *([] if spots is None else [spots]), *inputs
    )


def make_body(rows, cols):
    zs = rows // 2
    mate = [(r, r ^ 1) for r in range(rows)]

    def along(shift):
        return [(r, (r + 2 * shift) % rows) for r in range(rows)]

    def send(x, perm):
        return lax.ppermute(x, "row", perm)

    def cross(x, k):
        return lax.ppermute(x, "col", [(c, c ^ k) for c in range(cols)])

    def tree(parts):
        while len(parts) > 1:
            parts = [sum(parts[at : at + 2][1:], parts[at]) for at in range(0, len(parts), 2)]
        return parts[0]

    def over_z(x):
        perms = [[(r, r ^ (2 * k)) for r in range(rows)] for k in range(1, zs)]
        got = [send(x, perm) for perm in perms]
        return tree([x.astype(f32)] + [part.astype(f32) for part in got])

    def over_col(x):
        return tree([x.astype(f32)] + [cross(x, k).astype(f32) for k in range(1, cols)])

    def row_sum(x):
        return over_z(x + send(x, mate))

    def body(attn_out, out_cotangent, frozen, adapt_in, adapt_out, magnitude):
        layers, in_block, out_block = frozen.shape
        rank = adapt_in.shape[1]
        tokens = attn_out.shape[1] * cols
        mid = layers // 2
        row = lax.axis_index("row")
        col = lax.axis_index("col")
        core = row % 2
        z = row // 2
        step_at = zs // 2
        ups = [out_cotangent]
        downs = [out_cotangent]
        for _ in range(1, step_at):
            ups.append(send(ups[-1], along(1)))
            downs.append(send(downs[-1], along(-1)))
        acts = [attn_out] + [cross(attn_out, k) for k in range(1, cols)]
        far_up = send(ups[-1][:mid], along(1))
        far_down = send(downs[-1][mid:], along(-1))
        far = jnp.concatenate([far_up, far_down], 0)
        pieces = ups + downs[1:] + [far]
        places = [(z - at) % zs for at in range(step_at)]
        places += [(z + at) % zs for at in range(1, step_at)] + [(z + step_at) % zs]
        pieces = pieces + [send(piece, mate) for piece in pieces]
        spots = [p * 2 + core for p in places] + [p * 2 + 1 - core for p in places]
        spots = jnp.stack(spots + [col ^ k for k in range(cols)] + [core]).astype(jnp.int32)

        weights = (frozen, adapt_in, adapt_out)
        (squares,) = call(
            weight_stats,
            layers,
            None,
            list(weights),
            [jax.ShapeDtypeStruct((layers, 1, out_block), f32)],
        )
        squares = row_sum(squares)
        norms = jnp.sqrt(squares + 0.25)
        scales = magnitude[:, None, :] / norms

        *parts, dots, kept, given, in_part = call(
            lambda *refs: token_part(len(pieces), cols, *refs),
            layers,
            spots,
            pieces + acts + [*weights, scales],
            [jax.ShapeDtypeStruct((layers, tokens // cols, in_block), bf16)] * cols
            + [
                jax.ShapeDtypeStruct((layers, 1, out_block), f32),
                jax.ShapeDtypeStruct((layers, 2, rank // 2, out_block), f32),
                jax.ShapeDtypeStruct((layers, 2, rank // 2, out_block), bf16),
                jax.ShapeDtypeStruct((layers, rank, in_block), f32),
            ],
            [
                pltpu.VMEM((tokens, out_block), bf16),
                pltpu.VMEM((tokens, in_block), bf16),
                pltpu.VMEM((tokens, in_block), f32),
                pltpu.VMEM((2, rank, out_block), f32),
            ],
        )
        received = [parts[0]] + [cross(parts[k], k) for k in range(1, cols)]
        input_grad = tree([part.astype(f32) for part in received]).astype(bf16)
        dots = row_sum(dots)
        correct = -magnitude[:, None, :] * dots / (norms * norms * norms)
        magnitude_grad = (dots / norms)[:, 0]

        kept = kept + send(given, mate).astype(f32)
        kept = over_z(kept.astype(bf16))
        mine = kept[:, 0] * scales + kept[:, 1] * correct
        other = send(mine, mate)
        out_grad = jnp.where(
            core == 0, jnp.concatenate([mine, other], 1), jnp.concatenate([other, mine], 1)
        )

        (in_part,) = call(
            correct_part,
            layers,
            None,
            [*weights, correct, in_part],
            [jax.ShapeDtypeStruct((layers, rank, in_block), bf16)],
        )
        in_grad = over_col(in_part)
        return input_grad, in_grad, out_grad, magnitude_grad

    return body


def solution(mesh):
    return jax.shard_map(
        make_body(mesh.shape["row"], mesh.shape["col"]),
        mesh=mesh,
        in_specs=(
            P(None, "col", "row"),
            P(None, "row", "col"),
            P(None, "row", "col"),
            P(None, None, "row"),
            P(None, None, "col"),
            P(None, "col"),
        ),
        out_specs=(
            P(None, "col", "row"),
            P(None, None, "row"),
            P(None, None, "col"),
            P(None, "col"),
        ),
        check_vma=False,
    )
```
